256 devices in a mesh: groups: 4 (over x, y), feat: 64 (over z, core).
Axes of the slice: x: 2, y: 2, z: 32, core: 2. Of those that a mesh axis runs over, the one named last changes fastest.
The devices are a block of a 4x8x32 slice.
Arguments:
- cells: bfloat16 [768, 512, 192], P('groups', 'feat'), parts along dimension 0, may hold values from -6 to 6
- missing: int32 [768, 512], P('groups', 'feat'), parts along dimension 0, may hold values 0 or 1
- feat_ids: int32 [2048], P(('groups', 'feat')), parts along dimension 0, may hold values from 0 to 63
- feat_table: float32 [64, 192], replicated, may hold values from -5 to 5
- nan_embed: float32 [192], replicated, may hold values from -5 to 5
- gain_one: float32 [192], replicated, may hold values from 0.1 to 1.9
- w_qkv: bfloat16 [192, 576], replicated, may hold values from -3 to 3
- w_out: bfloat16 [192, 192], replicated, may hold values from -0.4375 to 0.4375
- gain_two: float32 [192], replicated, may hold values from 0.1 to 1.9
- w_up: bfloat16 [192, 768], replicated, may hold values from -0.4375 to 0.4375
- w_down: bfloat16 [768, 192], replicated, may hold values from -0.21875 to 0.21875
Outputs:
- result: float32 [768, 512, 192], P('groups', 'feat'), parts along dimension 0
The draws below stay inside these ranges and needn't reach their ends.
There are 4 independent parts, one for each index of `groups`. The reference program is written for one: setup_inputs(seed, part) draws one part's arguments, and reference() takes and returns one part's arrays. A program takes and returns all parts, laid end to end along the dimension named above; an argument that names none is the same for every part. Nothing has to cross between parts.
All inputs are finite; a program needn't handle non-finite values. No bound on the sum of `missing` on one device may be relied on, other than what follows from the above.
Results may differ from the reference program's by a relative error of at most 0.007.
The reference program's roundings to bfloat16 on the way (of `tokens`, `normed`, `qkv`, `probs`, `context`, `normed_two` and `act`) count: a program that leaves them out, or rounds other values in their place, can miss the bound.
Values may be sent and summed in bfloat16 or wider, within the bound.
No kernel may reach another device: no remote copies, remote signals or barrier semaphores. Data moves between devices by JAX's collectives and lax.ppermute only.
A program may use at most 64 MiB of HBM per device.

```python
import jax
import jax.numpy as jnp
from jax import lax

E = 192
HEADS = 6
MLP = 768
F = 512
NCAT = 64
R = 192


def draw_w_qkv(key, part):
    weights = jax.random.normal(key, (E, 3 * E), jnp.float32) * E ** (-0.5)
    return jnp.clip(weights, -3.0, 3.0).astype(jnp.bfloat16)


def touch_ends(values, key, smallest, top_value):
    longest = values.shape.index(max(values.shape))
    spots = []
    for shift in (0, 1):
        where = [jax.random.randint(jax.random.fold_in(key, axis), (), 0, length) for axis, length in enumerate(values.shape)]
        where[longest] = (where[longest] + shift) % values.shape[longest]
        spots.append(tuple(where))
    return values.at[spots[0]].set(smallest).at[spots[1]].set(top_value)


def block_scale(rng, extent, shards, smallest, high):
    def one(dim, parts):
        steps = jax.random.uniform(jax.random.fold_in(jax.random.fold_in(rng, 6), dim), (parts,), jnp.float32, smallest / len(shards), high / len(shards))
        return jnp.repeat(jnp.exp(steps), extent[dim] // parts).reshape((-1,) + (1,) * (len(extent) - dim - 1))

    loudness = one(*shards[0])
    for cut in shards[1:]:
        loudness = loudness * one(*cut)
    return loudness


def centred(stream_key, extent, spread, reach, pieces=(), held_as=jnp.bfloat16):
    drawn = jax.random.normal(stream_key, extent, jnp.float32) * spread
    if len(pieces) > 0:
        drawn = block_scale(stream_key, extent, pieces, -0.22, 0.18) * drawn
    return jnp.clip(drawn, min=-reach, max=reach).astype(held_as)


def setup_inputs(seed: int = 0, part: int = 0) -> dict:
    streams_of = jax.random.split(jax.random.key(seed), 12)
    part_splits = jax.random.split(jax.random.fold_in(streams_of[11], part), 12)
    return {
        "cells": centred(part_splits[0], (R, F, E), 1.0, 6.0, ((1, 64),)),
        "missing": touch_ends((jax.random.randint(part_splits[1], (R, F), 0, 4) < 1).astype(jnp.int32), jax.random.fold_in(part_splits[1], 1), 0, 1),
        "feat_ids": touch_ends(jax.random.randint(part_splits[2], (F,), 0, NCAT), jax.random.fold_in(part_splits[2], 1), 0, NCAT - 1).astype(jnp.int32),
        "feat_table": centred(streams_of[3], (NCAT, E), 0.7, 5.0, (), jnp.float32),
        "nan_embed": centred(streams_of[4], (E,), 1.0, 5.0, (), jnp.float32),
        "gain_one": jnp.clip(1.0 + 0.18 * jax.random.normal(streams_of[5], (E,), jnp.float32), 0.1, 1.9),
        "w_qkv": draw_w_qkv(jax.random.fold_in(streams_of[11], 71), part),
        "w_out": centred(streams_of[7], (E, E), E ** -0.5, 0.4375),
        "gain_two": jnp.clip(1.0 + 0.18 * jax.random.normal(streams_of[8], (E,), jnp.float32), 0.1, 1.9),
        "w_up": centred(streams_of[9], (E, MLP), E ** -0.5, 0.4375),
        "w_down": centred(streams_of[10], (MLP, E), MLP ** -0.5, 0.21875),
    }


def cell_norm(values, gain):
    mean = lax.optimization_barrier(jnp.mean(values, axis=-1, keepdims=True))
    centered = values - mean
    var = lax.optimization_barrier(jnp.mean(centered * centered, axis=-1, keepdims=True))
    return centered * lax.rsqrt(var + 1e-05) * gain

def attend(qkv):
    width = qkv.shape[-1] // 3
    count = qkv.shape[0]
    head_dim = width // HEADS
    query = qkv[:, :width].reshape(count, HEADS, head_dim).astype(jnp.float32)
    keys = qkv[:, width:2 * width].reshape(count, HEADS, head_dim).astype(jnp.float32)
    values = qkv[:, 2 * width:].reshape(count, HEADS, head_dim).astype(jnp.float32)
    scores = jnp.einsum('qhd,phd->hqp', query, keys) * head_dim ** (-0.5)
    top = lax.optimization_barrier(jnp.max(scores, axis=-1, keepdims=True))
    expo = jnp.exp(scores - top)
    probs = (expo / lax.optimization_barrier(jnp.sum(expo, axis=-1, keepdims=True))).astype(jnp.bfloat16)
    context = jnp.einsum('hqp,phd->qhd', probs.astype(jnp.float32), values)
    return context.astype(jnp.bfloat16).reshape(count, width)

def reference(cells, missing, feat_ids, feat_table, nan_embed, gain_one, w_qkv, w_out, gain_two, w_up, w_down):
    onehot = (feat_ids[:, None] == jnp.arange(NCAT, dtype=jnp.int32)[None, :]).astype(jnp.float32)
    femb = jnp.dot(onehot, feat_table, precision=lax.Precision.HIGHEST)
    tokens = (cells.astype(jnp.float32) + missing[..., None].astype(jnp.float32) * nan_embed + femb[None]).astype(jnp.bfloat16)

    def one_row(row):
        base = row.astype(jnp.float32)
        normed = cell_norm(base, gain_one).astype(jnp.bfloat16)
        qkv = jnp.dot(normed, w_qkv, preferred_element_type=jnp.float32).astype(jnp.bfloat16)
        context = attend(qkv)
        mid = base + jnp.dot(context, w_out, preferred_element_type=jnp.float32)
        normed_two = cell_norm(mid, gain_two).astype(jnp.bfloat16)
        act = jax.nn.gelu(jnp.dot(normed_two, w_up, preferred_element_type=jnp.float32), approximate=False).astype(jnp.bfloat16)
        return mid + jnp.dot(act, w_down, preferred_element_type=jnp.float32)
    return lax.map(one_row, tokens)
```

```python
import functools

import jax
import jax.numpy as jnp
from jax import lax
from jax.experimental import pallas as pl
from jax.experimental.pallas import tpu as pltpu
from jax.sharding import Mesh
from jax.sharding import PartitionSpec as P

HEADS = 6
LANES = 128
FEAT = ("chip", "core")
ALL = ("groups", "chip", "core")
F32 = jnp.float32
BF16 = jnp.bfloat16
NT = (((1,), (1,)), ((), ()))


def unpack(ref_rows, high_rows, side):
    low = ref_rows.astype(F32)
    high = high_rows.astype(F32)
    half = high.shape[-1] // 2
    low = low.reshape(-1, low.shape[-1])
    high = high.reshape(-1, high.shape[-1])
    return jnp.concatenate([low, high[:, side * half : (side + 1) * half]], axis=-1)


def normed_by(values, gain):
    width = values.shape[-1]
    mean = jnp.sum(values, axis=-1, keepdims=True) * (1.0 / width)
    centered = values - mean
    var = jnp.sum(centered * centered, axis=-1, keepdims=True) * (1.0 / width)
    return centered * lax.rsqrt(var + 1e-05) * gain


def pack_kernel(rows, ids_ref, cells_ref, missing_ref, table_ref, nan_ref, out_ref):
    feats, width = cells_ref.shape[1:]
    femb = jnp.concatenate([table_ref[pl.ds(ids_ref[f], 1), :] for f in range(feats)], axis=0)
    nan = nan_ref[...]
    chips = out_ref.shape[0]

    def tokens(r):
        column = missing_ref[:, r : r + 1].astype(F32)
        return cells_ref[r].astype(F32) + column * nan + femb

    for c in range(chips):
        for p in range(rows // 2):
            one, two = tokens(c * rows + 2 * p), tokens(c * rows + 2 * p + 1)
            both = jnp.concatenate([one[:, :LANES], two[:, :LANES]], axis=0)
            out_ref[c, 2 * p * feats : (2 * p + 2) * feats, :] = both.astype(BF16)
            high = jnp.concatenate([one[:, LANES:], two[:, LANES:]], axis=1)
            start = rows * feats + p * feats
            out_ref[c, start : start + feats, :] = high.astype(BF16)


def attention_kernel(rows, feats, own_ref, other_ref, gain_ref, w_ref, out_ref):
    width = gain_ref.shape[-1]
    head_dim = width // HEADS
    chips = own_ref.shape[0]
    cells = chips * feats
    head_of = lax.broadcasted_iota(jnp.int32, (1, width), 1) // head_dim
    scale = head_dim**-0.5 * 1.4426950408889634
    gain = gain_ref[...]

    @pl.loop(0, rows // 2)
    def _(p):
        highs = [r[:, pl.ds(pl.multiple_of((rows + p) * feats, feats), feats), :] for r in (own_ref, other_ref)]
        contexts = []
        for side in range(2):
            at = pl.ds(pl.multiple_of((2 * p + side) * feats, feats), feats)
            values = jnp.concatenate(
                [unpack(r[:, at, :], h, side) for r, h in zip((own_ref, other_ref), highs)], axis=0
            )
            normed = normed_by(values, gain).astype(BF16)
            q = jnp.dot(normed[:cells], w_ref[:, :width], preferred_element_type=F32)
            k = jnp.dot(normed, w_ref[:, width : 2 * width], preferred_element_type=F32).astype(BF16)
            v = jnp.dot(normed, w_ref[:, 2 * width :], preferred_element_type=F32).astype(BF16)
            q = q.astype(BF16)
            context = jnp.zeros((cells, width), F32)
            for h in range(HEADS):
                mine = head_of == h
                scores = lax.dot_general(
                    jnp.where(mine, q, jnp.zeros_like(q)), k, NT, preferred_element_type=F32
                )
                top = jnp.max(scores, axis=-1, keepdims=True)
                expo = jnp.exp2((scores - top) * scale)
                total = jnp.sum(expo, axis=-1, keepdims=True)
                part = jnp.dot(expo.astype(BF16), v, preferred_element_type=F32)
                context = jnp.where(mine, part / total, context)
            out_ref[:, at, :] = context[:, :LANES].reshape(chips, feats, LANES).astype(BF16)
            contexts.append(context[:, LANES:])
        high = jnp.concatenate(contexts, axis=1).reshape(chips, feats, LANES)
        out_ref[:, pl.ds(pl.multiple_of((rows + p) * feats, feats), feats), :] = high.astype(BF16)


def finish_kernel(rows, feats, base_ref, context_ref, w_out_ref, gain_ref, w_up_ref, w_down_ref, out_ref):
    width = gain_ref.shape[-1]
    chips = base_ref.shape[0]

    def whole(ref):
        low = ref[:, : rows * feats, :].astype(F32).reshape(chips, rows // 2, 2, feats, LANES)
        high = ref[:, rows * feats :, :].astype(F32).reshape(chips, rows // 2, feats, LANES)
        half = LANES // 2
        sides = [
            jnp.concatenate([low[:, :, s], high[..., s * half : (s + 1) * half]], axis=-1) for s in range(2)
        ]
        return jnp.stack(sides, axis=2).reshape(-1, width)

    context = whole(context_ref).astype(BF16)
    mid = whole(base_ref) + jnp.dot(context, w_out_ref[...], preferred_element_type=F32)
    normed = normed_by(mid, gain_ref[...]).astype(BF16)
    up = jnp.dot(normed, w_up_ref[...], preferred_element_type=F32)
    act = (0.5 * up * (1.0 + lax.erf(up * 0.5**0.5))).astype(BF16)
    out = mid + lax.dot_general(act, w_down_ref[...], NT, preferred_element_type=F32)
    out_ref[...] = out.reshape(out_ref.shape)


def vmem(count):
    return [pl.BlockSpec(memory_space=pltpu.VMEM)] * count


def body(
    cells, missing, feat_ids, feat_table, nan_embed, gain_one, w_qkv, w_out, gain_two, w_up, w_down
):
    chips = lax.axis_size("chip")
    all_rows, feats, width = cells.shape
    rows = all_rows // chips
    packed = jax.ShapeDtypeStruct((chips, rows * feats * width // LANES, LANES), BF16)
    tokens = pl.pallas_call(
        functools.partial(pack_kernel, rows),
        out_shape=packed,
        in_specs=[pl.BlockSpec(memory_space=pltpu.SMEM), *vmem(4)],
        out_specs=vmem(1)[0],
        name="pack",
    )(feat_ids, cells, missing.T, feat_table, nan_embed[None])
    own = lax.all_to_all(tokens, "chip", 0, 0, tiled=True)
    other = lax.ppermute(own, "core", [(0, 1), (1, 0)])
    context = pl.pallas_call(
        functools.partial(attention_kernel, rows, feats),
        out_shape=packed,
        in_specs=vmem(4),
        out_specs=vmem(1)[0],
        name="attend",
    )(own, other, gain_one[None], w_qkv)
    context = lax.all_to_all(context, "chip", 0, 0, tiled=True)
    steps = 4 if chips % 4 == 0 else 1
    block = (chips // steps, *packed.shape[1:])
    whole = lambda shape: pl.BlockSpec(shape, lambda i: (0, 0))
    return pl.pallas_call(
        functools.partial(finish_kernel, rows, feats),
        out_shape=jax.ShapeDtypeStruct(cells.shape, F32),
        grid=(steps,),
        in_specs=[
            pl.BlockSpec(block, lambda i: (i, 0, 0)),
            pl.BlockSpec(block, lambda i: (i, 0, 0)),
            whole(w_out.shape),
            whole((1, width)),
            whole(w_up.shape),
            whole(w_down.shape[::-1]),
        ],
        out_specs=pl.BlockSpec((all_rows // steps, feats, width), lambda i: (i, 0, 0)),
        name="finish",
    )(tokens, context, w_out, gain_two[None], w_up, w_down.T)


def solution(mesh):
    chips = mesh.shape["feat"] // 2
    split = Mesh(mesh.devices.reshape(mesh.shape["groups"], chips, 2), ALL)
    in_specs = (P("groups", FEAT, None), P("groups", FEAT), P(ALL)) + (P(),) * 8
    return jax.shard_map(
        body, mesh=split, in_specs=in_specs, out_specs=P("groups", FEAT, None), check_vma=False
    )
```

```python
import functools

import jax
import jax.numpy as jnp
from jax import lax
from jax.experimental import pallas as pl
from jax.experimental.pallas import tpu as pltpu
from jax.sharding import Mesh
from jax.sharding import PartitionSpec as P

HEADS = 6
LANES = 128
ONES = 16
LEAD, LAG = 2, 1
HOLD_NS = 27000
FEAT = ("chip", "core")
ALL = ("groups", "chip", "core")
F32 = jnp.float32
BF16 = jnp.bfloat16
NT = (((1,), (1,)), ((), ()))


def normed_by(values, gain):
    width = values.shape[-1]
    mean = jnp.sum(values, axis=-1, keepdims=True) * (1.0 / width)
    centered = values - mean
    var = jnp.sum(centered * centered, axis=-1, keepdims=True) * (1.0 / width)
    return centered * lax.rsqrt(var + 1e-05) * gain


def tokens_kernel(chips, cells_ref, missing_ref, table_ref, nan_ref, ids_ref, own_ref, other_ref):
    feats = cells_ref.shape[1]
    rows = cells_ref.shape[0] // chips
    half = rows // 2
    core = lax.axis_index("core")
    femb = jnp.concatenate([table_ref[pl.ds(ids_ref[f], 1), :] for f in range(feats)], axis=0)
    nan = nan_ref[...]
    low = missing_ref[...].astype(F32)
    high = jnp.concatenate([low[:, half:], low[:, :half]], axis=1)
    for j, out_ref in enumerate((own_ref, other_ref)):
        of_core = core if j == 0 else 1 - core
        column = jnp.where(of_core == 0, low, high)
        for c in range(chips):
            for i in range(half):
                lane = c * rows + i
                cell = cells_ref[lane + of_core * half].astype(F32)
                out_ref[c * half + i] = (cell + column[:, lane : lane + 1] * nan + femb).astype(BF16)


def merge_kernel(own_ref, other_ref, out_ref):
    chips = out_ref.shape[0]
    half = own_ref.shape[0] // chips
    feats = own_ref.shape[1]

    @pl.when(lax.axis_index("core") == 1)
    def _():
        pl.delay(HOLD_NS)

    for c in range(chips):
        for i in range(half):
            own = own_ref[c * half + i].astype(F32)
            other = other_ref[c * half + i].astype(F32)
            low = jnp.concatenate([own[:, :LANES], other[:, :LANES]], axis=0).astype(BF16)
            high = jnp.concatenate([own[:, LANES:], other[:, LANES:]], axis=1).astype(BF16)
            out_ref[c, 3 * i * feats : (3 * i + 2) * feats, :] = low
            out_ref[c, (3 * i + 2) * feats : (3 * i + 3) * feats, :] = high


def attention_kernel(feats, in_ref, gain_ref, w_ref, w_v_ref, out_ref):
    width = gain_ref.shape[-1]
    head_dim = width // HEADS
    chips = in_ref.shape[0]
    cells = chips * feats
    split = LANES // 2
    head_of = lax.broadcasted_iota(jnp.int32, (1, width), 1) // head_dim
    scale = head_dim**-0.5 * 1.4426950408889634
    gain = gain_ref[...]

    def tile(i, t):
        return pl.ds(pl.multiple_of((3 * i + t) * feats, feats), feats)

    def flat(i, t):
        return in_ref[:, tile(i, t), :].astype(F32).reshape(cells, LANES)

    def scores_of(q, k, h):
        mine = jnp.where(head_of == h, q, jnp.zeros_like(q))
        return lax.dot_general(k, mine, NT, preferred_element_type=F32)

    def softmax(s):
        top = jnp.max(s, axis=0, keepdims=True)
        return jnp.exp2((s - top) * scale).astype(BF16)

    def context_of(v, expo, h):
        mine = v[h * head_dim : (h + 1) * head_dim]
        mine = jnp.concatenate([mine, jnp.ones((ONES, 2 * cells), BF16)], axis=0)
        part = jnp.dot(mine, expo, preferred_element_type=F32)
        return part[:head_dim] * (1.0 / part[head_dim : head_dim + 1])

    @pl.loop(0, in_ref.shape[1] // (3 * feats))
    def _(i):
        high = flat(i, 2)
        values = jnp.concatenate(
            [
                jnp.concatenate([flat(i, side), high[:, side * split : (side + 1) * split]], axis=1)
                for side in range(2)
            ],
            axis=0,
        )
        normed = normed_by(values, gain).astype(BF16)
        q = jnp.dot(normed, w_ref[:, :width], preferred_element_type=F32).astype(BF16)
        k = jnp.dot(normed, w_ref[:, width:], preferred_element_type=F32).astype(BF16)
        v = lax.dot_general(w_v_ref[...], normed, NT, preferred_element_type=F32).astype(BF16)
        sides = [q[:cells], q[cells:]]
        pairs = [(h, side) for h in range(HEADS) for side in range(2)]
        ahead = [scores_of(sides[side], k, h) for h, side in pairs[:LEAD]]
        done = [[], []]
        expos = []
        for n, (h, side) in enumerate(pairs):
            if n + LEAD < len(pairs):
                h2, side2 = pairs[n + LEAD]
                ahead.append(scores_of(sides[side2], k, h2))
            expos.append(softmax(ahead.pop(0)))
            if n >= LAG:
                h0, side0 = pairs[n - LAG]
                done[side0].append(context_of(v, expos.pop(0), h0))
        for h0, side0 in pairs[len(pairs) - LAG :]:
            done[side0].append(context_of(v, expos.pop(0), h0))
        highs = []
        for side in range(2):
            done[side].append(jnp.zeros((2 * LANES - width, cells), F32))
            context = jnp.concatenate(done[side], axis=0).T
            out_ref[:, tile(i, side), :] = context[:, :LANES].reshape(chips, feats, LANES).astype(BF16)
            highs.append(context[:, LANES:width])
        high = jnp.concatenate(highs, axis=1).reshape(chips, feats, LANES)
        out_ref[:, tile(i, 2), :] = high.astype(BF16)


def finish_kernel(
    feats, own_base_ref, other_base_ref, own_ref, other_ref, w_out_ref, gain_ref, w_up_ref, w_down_ref, out_ref
):
    width = gain_ref.shape[-1]
    chips = own_ref.shape[0]
    half = own_ref.shape[1] // (3 * feats)
    split = LANES // 2
    core = lax.axis_index("core")
    for j, (base_ref, context_ref) in enumerate(((own_base_ref, own_ref), (other_base_ref, other_ref))):
        tiles = context_ref[...].astype(F32).reshape(chips, half, 3, feats, LANES)
        context = jnp.concatenate([tiles[:, :, j], tiles[:, :, 2, :, j * split : (j + 1) * split]], axis=-1)
        context = context.reshape(-1, width).astype(BF16)
        base = base_ref[...].astype(F32).reshape(-1, width)
        mid = base + jnp.dot(context, w_out_ref[...], preferred_element_type=F32)
        normed = normed_by(mid, gain_ref[...]).astype(BF16)
        up = jnp.dot(normed, w_up_ref[...], preferred_element_type=F32)
        act = (0.5 * up * (1.0 + lax.erf(up * 0.5**0.5))).astype(BF16)
        out = mid + lax.dot_general(act, w_down_ref[...], NT, preferred_element_type=F32)
        out = out.reshape(chips, half, feats, width)
        of_core = core if j == 0 else 1 - core
        for c in range(chips):
            out_ref[pl.ds(c * 2 * half + of_core * half, half)] = out[c]


def vmem(count):
    return [pl.BlockSpec(memory_space=pltpu.VMEM)] * count


def limit(mib):
    return pltpu.CompilerParams(vmem_limit_bytes=mib << 20)


def body(
    cells, missing, feat_ids, feat_table, nan_embed, gain_one, w_qkv, w_out, gain_two, w_up, w_down
):
    chips = lax.axis_size("chip")
    all_rows, feats, width = cells.shape
    swap = [(0, 1), (1, 0)]
    halves = jax.ShapeDtypeStruct((all_rows // 2, feats, width), BF16)
    packed = jax.ShapeDtypeStruct((chips, all_rows * feats * width // (chips * LANES), LANES), BF16)
    own, other = pl.pallas_call(
        functools.partial(tokens_kernel, chips),
        out_shape=[halves] * 2,
        in_specs=[*vmem(4), pl.BlockSpec(memory_space=pltpu.SMEM)],
        out_specs=vmem(2),
        name="tokens",
    )(cells, missing.T, feat_table, nan_embed[None], feat_ids)
    tokens = pl.pallas_call(
        merge_kernel,
        out_shape=packed,
        in_specs=vmem(2),
        out_specs=vmem(1)[0],
        compiler_params=limit(12),
        name="merge",
    )(own, lax.ppermute(other, "core", swap))
    tokens = lax.all_to_all(tokens, "chip", 0, 0, tiled=True)
    context = pl.pallas_call(
        functools.partial(attention_kernel, feats),
        out_shape=packed,
        in_specs=vmem(4),
        out_specs=vmem(1)[0],
        compiler_params=limit(24),
        name="attend",
    )(tokens, gain_one[None], w_qkv[:, : 2 * width], w_qkv[:, 2 * width :].T)
    context = lax.all_to_all(context, "chip", 0, 0, tiled=True)
    steps = 4 if chips % 4 == 0 else 1
    some = pl.BlockSpec((chips // steps, *packed.shape[1:]), lambda n: (n, 0, 0))
    base = pl.BlockSpec((all_rows // 2 // steps, feats, width), lambda n: (n, 0, 0))
    whole = lambda shape: pl.BlockSpec(shape, lambda n: (0, 0))
    return pl.pallas_call(
        functools.partial(finish_kernel, feats),
        out_shape=jax.ShapeDtypeStruct(cells.shape, F32),
        grid=(steps,),
        in_specs=[
            *[base] * 2,
            *[some] * 2,
            whole(w_out.shape),
            whole((1, width)),
            whole(w_up.shape),
            whole(w_down.shape[::-1]),
        ],
        out_specs=pl.BlockSpec((all_rows // steps, feats, width), lambda n: (n, 0, 0)),
        compiler_params=limit(16),
        name="finish",
    )(own, other, context, lax.ppermute(context, "core", swap), w_out, gain_two[None], w_up, w_down.T)


def solution(mesh):
    chips = mesh.shape["feat"] // 2
    split = Mesh(mesh.devices.reshape(mesh.shape["groups"], chips, 2), ALL)
    in_specs = (P("groups", FEAT, None), P("groups", FEAT), P(ALL)) + (P(),) * 8
    return jax.shard_map(
        body, mesh=split, in_specs=in_specs, out_specs=P("groups", FEAT, None), check_vma=False
    )
```

```python
import functools

import jax
import jax.numpy as jnp
from jax import lax
from jax.experimental import pallas as pl
from jax.experimental.pallas import tpu as pltpu
from jax.sharding import Mesh
from jax.sharding import PartitionSpec as P

HEADS = 6
LANES = 128
ONES = 16
LEAD, LAG = 2, 1
HOLD_NS = 28000
PIECES = 4
FEAT = ("chip", "core")
ALL = ("groups", "chip", "core")
F32 = jnp.float32
BF16 = jnp.bfloat16
NT = (((1,), (1,)), ((), ()))
TT = (((0,), (1,)), ((), ()))


def normed_by(values, gain):
    width = values.shape[-1]
    mean = jnp.sum(values, axis=-1, keepdims=True) * (1.0 / width)
    centered = values - mean
    var = jnp.sum(centered * centered, axis=-1, keepdims=True) * (1.0 / width)
    return centered * lax.rsqrt(var + 1e-05) * gain


def tokens_kernel(
    chips, cells_hbm, missing_hbm, table_hbm, nan_hbm, ids_hbm, own_ref, other_ref,
    cells_ref, missing_ref, table_ref, nan_ref, ids_ref, sems
):
    feats = cells_ref.shape[1]
    rows = cells_ref.shape[0] // chips
    half = rows // 2
    part = cells_ref.shape[0] // PIECES
    core = lax.axis_index("core")
    small = [
        pltpu.make_async_copy(*pair, sems.at[n])
        for n, pair in enumerate(
            [(ids_hbm, ids_ref), (table_hbm, table_ref), (missing_hbm, missing_ref), (nan_hbm, nan_ref)]
        )
    ]
    large = [
        pltpu.make_async_copy(
            cells_hbm.at[pl.ds(n * part, part)], cells_ref.at[pl.ds(n * part, part)], sems.at[len(small) + n]
        )
        for n in range(PIECES)
    ]
    for copy in small + large:
        copy.start()
    for copy in small:
        copy.wait()
    femb = jnp.concatenate([table_ref[pl.ds(ids_ref[f], 1), :] for f in range(feats)], axis=0)
    nan = nan_ref[...]
    low = missing_ref[...].astype(F32)
    high = jnp.concatenate([low[:, half:], low[:, :half]], axis=1)
    columns = [jnp.where(c == 0, low, high) for c in (core, 1 - core)]
    for c in range(chips):
        if c % (chips // PIECES) == 0:
            large[c // (chips // PIECES)].wait()
        for of_core, column, out_ref in ((core, columns[0], own_ref), (1 - core, columns[1], other_ref)):
            for i in range(half):
                lane = c * rows + i
                cell = cells_ref[lane + of_core * half].astype(F32)
                out_ref[c * half + i] = (cell + column[:, lane : lane + 1] * nan + femb).astype(BF16)


def merge_kernel(own_ref, other_ref, out_ref):
    chips = out_ref.shape[0]
    half = own_ref.shape[0] // chips
    feats = own_ref.shape[1]

    @pl.when(lax.axis_index("core") == 1)
    def _():
        pl.delay(HOLD_NS)

    for c in range(chips):
        for i in range(half):
            own = own_ref[c * half + i].astype(F32)
            other = other_ref[c * half + i].astype(F32)
            low = jnp.concatenate([own[:, :LANES], other[:, :LANES]], axis=0).astype(BF16)
            high = jnp.concatenate([own[:, LANES:], other[:, LANES:]], axis=1).astype(BF16)
            out_ref[c, 3 * i * feats : (3 * i + 2) * feats, :] = low
            out_ref[c, (3 * i + 2) * feats : (3 * i + 3) * feats, :] = high


def attention_kernel(feats, in_ref, gain_ref, w_ref, out_ref):
    width = gain_ref.shape[-1]
    head_dim = width // HEADS
    chips = in_ref.shape[0]
    cells = chips * feats
    split = LANES // 2
    head_of = lax.broadcasted_iota(jnp.int32, (1, width), 1) // head_dim
    scale = head_dim**-0.5 * 1.4426950408889634
    gain = gain_ref[...]

    def tile(i, t):
        return pl.ds(pl.multiple_of((3 * i + t) * feats, feats), feats)

    def flat(i, t):
        return in_ref[:, tile(i, t), :].astype(F32).reshape(cells, LANES)

    def scores_of(q, k, h):
        mine = jnp.where(head_of == h, q, jnp.zeros_like(q))
        return lax.dot_general(k, mine, NT, preferred_element_type=F32)

    def softmax(s):
        top = jnp.max(s, axis=0, keepdims=True)
        return jnp.exp2((s - top) * scale).astype(BF16)

    def context_of(v, expo, h):
        mine = v[h * head_dim : (h + 1) * head_dim]
        mine = jnp.concatenate([mine, jnp.ones((ONES, 2 * cells), BF16)], axis=0)
        part = jnp.dot(mine, expo, preferred_element_type=F32)
        return part[:head_dim] * (1.0 / part[head_dim : head_dim + 1])

    @pl.loop(0, in_ref.shape[1] // (3 * feats))
    def _(i):
        high = flat(i, 2)
        values = jnp.concatenate(
            [
                jnp.concatenate([flat(i, side), high[:, side * split : (side + 1) * split]], axis=1)
                for side in range(2)
            ],
            axis=0,
        )
        normed = normed_by(values, gain).astype(BF16)
        q = jnp.dot(normed, w_ref[:, :width], preferred_element_type=F32).astype(BF16)
        k = jnp.dot(normed, w_ref[:, width : 2 * width], preferred_element_type=F32).astype(BF16)
        v = lax.dot_general(w_ref[:, 2 * width :], normed, TT, preferred_element_type=F32).astype(BF16)
        sides = [q[:cells], q[cells:]]
        pairs = [(h, side) for h in range(HEADS) for side in range(2)]
        ahead = [scores_of(sides[side], k, h) for h, side in pairs[:LEAD]]
        done = [[], []]
        expos = []
        for n, (h, side) in enumerate(pairs):
            if n + LEAD < len(pairs):
                h2, side2 = pairs[n + LEAD]
                ahead.append(scores_of(sides[side2], k, h2))
            expos.append(softmax(ahead.pop(0)))
            if n >= LAG:
                h0, side0 = pairs[n - LAG]
                done[side0].append(context_of(v, expos.pop(0), h0))
        for h0, side0 in pairs[len(pairs) - LAG :]:
            done[side0].append(context_of(v, expos.pop(0), h0))
        highs = []
        for side in range(2):
            done[side].append(jnp.zeros((2 * LANES - width, cells), F32))
            context = jnp.concatenate(done[side], axis=0).T
            out_ref[:, tile(i, side), :] = context[:, :LANES].reshape(chips, feats, LANES).astype(BF16)
            highs.append(context[:, LANES:width])
        high = jnp.concatenate(highs, axis=1).reshape(chips, feats, LANES)
        out_ref[:, tile(i, 2), :] = high.astype(BF16)


def finish_kernel(
    feats, of_other, base_ref, context_ref, w_out_ref, gain_ref, w_up_ref, w_down_ref, *rest
):
    out_hbm, held_ref, sems = rest[-3:]
    width = gain_ref.shape[-1]
    chips = context_ref.shape[0]
    half = context_ref.shape[1] // (3 * feats)
    split = LANES // 2
    core = lax.axis_index("core")
    of_core = 1 - core if of_other else core
    part = chips // PIECES
    copies = []
    for n in range(PIECES):
        tiles = context_ref[n * part : (n + 1) * part].astype(F32).reshape(part, half, 3, feats, LANES)
        high = tiles[:, :, 2, :, of_other * split : (of_other + 1) * split]
        context = jnp.concatenate([tiles[:, :, of_other], high], axis=-1).reshape(-1, width)
        base = base_ref[n * part * half : (n + 1) * part * half].astype(F32).reshape(-1, width)
        mid = base + jnp.dot(context.astype(BF16), w_out_ref[...], preferred_element_type=F32)
        normed = normed_by(mid, gain_ref[...]).astype(BF16)
        up = jnp.dot(normed, w_up_ref[...], preferred_element_type=F32)
        act = (0.5 * up * (1.0 + lax.erf(up * 0.5**0.5))).astype(BF16)
        out = mid + lax.dot_general(act, w_down_ref[...], NT, preferred_element_type=F32)
        at = pl.ds(n * part, part)
        held_ref[n * part : (n + 1) * part] = out.reshape(part, half, feats, width)
        copies.append(pltpu.make_async_copy(held_ref.at[at], out_hbm.at[at, of_core], sems.at[n]))
        copies[-1].start()
    for copy in copies:
        copy.wait()


def vmem(count):
    return [pl.BlockSpec(memory_space=pltpu.VMEM)] * count


def limit(mib):
    return pltpu.CompilerParams(vmem_limit_bytes=mib << 20)


def body(
    cells, missing, feat_ids, feat_table, nan_embed, gain_one, w_qkv, w_out, gain_two, w_up, w_down
):
    chips = lax.axis_size("chip")
    all_rows, feats, width = cells.shape
    swap = [(0, 1), (1, 0)]
    halves = jax.ShapeDtypeStruct((all_rows // 2, feats, width), BF16)
    packed = jax.ShapeDtypeStruct((chips, all_rows * feats * width // (chips * LANES), LANES), BF16)
    hbm = pl.BlockSpec(memory_space=pltpu.HBM)
    own, other = pl.pallas_call(
        functools.partial(tokens_kernel, chips),
        out_shape=[halves] * 2,
        in_specs=[hbm] * 5,
        out_specs=vmem(2),
        scratch_shapes=[
            pltpu.VMEM(cells.shape, cells.dtype),
            pltpu.VMEM(missing.shape[::-1], missing.dtype),
            pltpu.VMEM(feat_table.shape, F32),
            pltpu.VMEM((1, width), F32),
            pltpu.SMEM(feat_ids.shape, feat_ids.dtype),
            pltpu.SemaphoreType.DMA((4 + PIECES,)),
        ],
        compiler_params=limit(12),
        name="tokens",
    )(*(pltpu.with_memory_space_constraint(x, pltpu.HBM) for x in (cells, missing.T, feat_table, nan_embed[None], feat_ids)))
    tokens = pl.pallas_call(
        merge_kernel,
        out_shape=packed,
        in_specs=vmem(2),
        out_specs=vmem(1)[0],
        compiler_params=limit(12),
        name="merge",
    )(own, lax.ppermute(other, "core", swap))
    tokens = lax.all_to_all(tokens, "chip", 0, 0, tiled=True)
    context = pl.pallas_call(
        functools.partial(attention_kernel, feats),
        out_shape=packed,
        in_specs=vmem(3),
        out_specs=vmem(1)[0],
        compiler_params=limit(24),
        name="attend",
    )(tokens, gain_one[None], w_qkv)
    context = lax.all_to_all(context, "chip", 0, 0, tiled=True)
    swapped = lax.ppermute(context, "core", swap)
    half = all_rows // chips // 2
    result = jax.ShapeDtypeStruct((chips, 2, half, feats, width), F32)

    def finish(of_other, base, context, *before):
        return pl.pallas_call(
            functools.partial(finish_kernel, feats, of_other),
            out_shape=result,
            in_specs=[*vmem(6), *[hbm] * len(before)],
            out_specs=hbm,
            scratch_shapes=[
                pltpu.VMEM((chips, half, feats, width), F32),
                pltpu.SemaphoreType.DMA((PIECES,)),
            ],
            input_output_aliases={6: 0} if before else {},
            compiler_params=limit(16),
            cost_estimate=pl.CostEstimate(flops=10**9, bytes_accessed=2 * 10**6, transcendentals=0),
            name="finish",
        )(base, context, w_out, gain_two[None], w_up, w_down.T, *before)

    return finish(1, other, swapped, finish(0, own, context)).reshape(cells.shape)


def solution(mesh):
    chips = mesh.shape["feat"] // 2
    split = Mesh(mesh.devices.reshape(mesh.shape["groups"], chips, 2), ALL)
    in_specs = (P("groups", FEAT, None), P("groups", FEAT), P(ALL)) + (P(),) * 8
    return jax.shard_map(
        body, mesh=split, in_specs=in_specs, out_specs=P("groups", FEAT, None), check_vma=False
    )
```

```python
import functools

import jax
import jax.numpy as jnp
from jax import lax
from jax.experimental import pallas as pl
from jax.experimental.pallas import tpu as pltpu
from jax.sharding import Mesh
from jax.sharding import PartitionSpec as P

HEADS = 6
LANES = 128
ONES = 16
LEAD, LAG = 2,1
EARLY = 1
HOLD_NS = 27000
PIECES = 4
FEAT = ("chip", "core")
ALL = ("groups", "chip", "core")
F32 = jnp.float32
BF16 = jnp.bfloat16
NT = (((1,), (1,)), ((), ()))
TT = (((0,), (1,)), ((), ()))


def normed_by(values, gain):
    width = values.shape[-1]
    mean = jnp.sum(values, axis=-1, keepdims=True) * (1.0 / width)
    centered = values - mean
    var = jnp.sum(centered * centered, axis=-1, keepdims=True) * (1.0 / width)
    return centered * lax.rsqrt(var + 1e-05) * gain


def tokens_kernel(
    chips, cells_hbm, missing_hbm, table_hbm, nan_hbm, ids_hbm, own_ref, other_ref,
    cells_ref, missing_ref, table_ref, nan_ref, ids_ref, sems
):
    feats = cells_ref.shape[1]
    rows = cells_ref.shape[0] // chips
    half = rows // 2
    part = cells_ref.shape[0] // PIECES
    core = lax.axis_index("core")
    small = [
        pltpu.make_async_copy(*pair, sems.at[n])
        for n, pair in enumerate(
            [(ids_hbm, ids_ref), (table_hbm, table_ref), (missing_hbm, missing_ref), (nan_hbm, nan_ref)]
        )
    ]
    large = [
        pltpu.make_async_copy(
            cells_hbm.at[pl.ds(n * part, part)], cells_ref.at[pl.ds(n * part, part)], sems.at[len(small) + n]
        )
        for n in range(PIECES)
    ]
    for copy in small + large:
        copy.start()
    for copy in small:
        copy.wait()
    femb = jnp.concatenate([table_ref[pl.ds(ids_ref[f], 1), :] for f in range(feats)], axis=0)
    nan = nan_ref[...]
    low = missing_ref[...].astype(F32)
    high = jnp.concatenate([low[:, half:], low[:, :half]], axis=1)
    columns = [jnp.where(c == 0, low, high) for c in (core, 1 - core)]
    for c in range(chips):
        if c % (chips // PIECES) == 0:
            large[c // (chips // PIECES)].wait()
        for of_core, column, out_ref in ((core, columns[0], own_ref), (1 - core, columns[1], other_ref)):
            for i in range(half):
                lane = c * rows + i
                cell = cells_ref[lane + of_core * half].astype(F32)
                out_ref[c * half + i] = (cell + column[:, lane : lane + 1] * nan + femb).astype(BF16)


def merge_kernel(own_ref, other_ref, out_ref):
    chips = out_ref.shape[0]
    half = own_ref.shape[0] // chips
    feats = own_ref.shape[1]

    @pl.when(lax.axis_index("core") == 1)
    def _():
        pl.delay(HOLD_NS)

    for c in range(chips):
        for i in range(half):
            own = own_ref[c * half + i].astype(F32)
            other = other_ref[c * half + i].astype(F32)
            low = jnp.concatenate([own[:, :LANES], other[:, :LANES]], axis=0).astype(BF16)
            high = jnp.concatenate([own[:, LANES:], other[:, LANES:]], axis=1).astype(BF16)
            out_ref[c, 3 * i * feats : (3 * i + 2) * feats, :] = low
            out_ref[c, (3 * i + 2) * feats : (3 * i + 3) * feats, :] = high


def attention_kernel(feats, in_ref, gain_ref, w_ref, out_ref):
    width = gain_ref.shape[-1]
    head_dim = width // HEADS
    chips = in_ref.shape[0]
    cells = chips * feats
    split = LANES // 2
    head_of = lax.broadcasted_iota(jnp.int32, (1, width), 1) // head_dim
    scale = head_dim**-0.5 * 1.4426950408889634
    gain = gain_ref[...]

    def tile(i, t):
        return pl.ds(pl.multiple_of((3 * i + t) * feats, feats), feats)

    def flat(i, t):
        return in_ref[:, tile(i, t), :].astype(F32).reshape(cells, LANES)

    def scores_of(q, k, h):
        mine = jnp.where(head_of == h, q, jnp.zeros_like(q))
        return lax.dot_general(k, mine, NT, preferred_element_type=F32)

    def softmax(s):
        top = jnp.max(s, axis=0, keepdims=True)
        return jnp.exp2((s - top) * scale).astype(BF16)

    def context_of(v, expo, h):
        mine = v[h * head_dim : (h + 1) * head_dim]
        mine = jnp.concatenate([mine, jnp.ones((ONES, 2 * cells), BF16)], axis=0)
        part = jnp.dot(mine, expo, preferred_element_type=F32)
        return part[:head_dim] * (1.0 / part[head_dim : head_dim + 1])

    def ready(i):
        high = flat(i, 2)
        values = jnp.concatenate(
            [
                jnp.concatenate([flat(i, side), high[:, side * split : (side + 1) * split]], axis=1)
                for side in range(2)
            ],
            axis=0,
        )
        normed = normed_by(values, gain).astype(BF16)
        q = jnp.dot(normed, w_ref[:, :width], preferred_element_type=F32).astype(BF16)
        k = jnp.dot(normed, w_ref[:, width : 2 * width], preferred_element_type=F32).astype(BF16)
        v = lax.dot_general(w_ref[:, 2 * width :], normed, TT, preferred_element_type=F32).astype(BF16)
        return (q[:cells], q[cells:]), k, v

    def put(i, done):
        highs = []
        for side in range(2):
            rest = jnp.zeros((2 * LANES - width, cells), F32)
            context = jnp.concatenate([*done[side], rest], axis=0).T
            out_ref[:, tile(i, side), :] = context[:, :LANES].reshape(chips, feats, LANES).astype(BF16)
            highs.append(context[:, LANES:width])
        high = jnp.concatenate(highs, axis=1).reshape(chips, feats, LANES)
        out_ref[:, tile(i, 2), :] = high.astype(BF16)

    count = in_ref.shape[1] // (3 * feats)
    units = [(i, h, side) for i in range(count) for h in range(HEADS) for side in range(2)]
    made = {0: ready(0)}
    done = {(i, side): [] for i in range(count) for side in range(2)}
    ahead, expos = [], []

    def issue(n):
        i, h, side = units[n]
        ahead.append(scores_of(made[i][0][side], made[i][1], h))

    def retire(n):
        i, h, side = units[n]
        done[i, side].append(context_of(made[i][2], expos.pop(0), h))
        if (h, side) == (HEADS - 1, 1):
            put(i, [done[i, 0], done[i, 1]])

    for n in range(LEAD):
        issue(n)
    for n, (i, h, side) in enumerate(units):
        if (h, side) == (EARLY, 0) and i + 1 < count:
            made[i + 1] = ready(i + 1)
        if n + LEAD < len(units):
            issue(n + LEAD)
        expos.append(softmax(ahead.pop(0)))
        if n >= LAG:
            retire(n - LAG)
    for n in range(len(units) - LAG, len(units)):
        retire(n)


def finish_kernel(
    feats, of_other, base_ref, context_ref, w_out_ref, gain_ref, w_up_ref, w_down_ref, *rest
):
    width = gain_ref.shape[-1]
    chips = context_ref.shape[0]
    half = context_ref.shape[1] // (3 * feats)
    split = LANES // 2
    core = lax.axis_index("core")
    pieces = PIECES if of_other else 2
    part = chips // pieces
    copies = []

    def copy_out(source, n, of_core):
        at = pl.ds(n * part, part)
        copies.append(pltpu.make_async_copy(source.at[at], out_hbm.at[at, of_core], sems.at[len(copies)]))
        copies[-1].start()

    if of_other:
        first_ref, out_hbm, held_ref, sems = rest
        for n in range(pieces):
            copy_out(first_ref, n, core)
    else:
        (held_ref,) = rest

    def start(n):
        tiles = context_ref[n * part : (n + 1) * part].astype(F32).reshape(part, half, 3, feats, LANES)
        high = tiles[:, :, 2, :, of_other * split : (of_other + 1) * split]
        context = jnp.concatenate([tiles[:, :, of_other], high], axis=-1).reshape(-1, width)
        base = base_ref[n * part * half : (n + 1) * part * half].astype(F32).reshape(-1, width)
        mid = base + jnp.dot(context.astype(BF16), w_out_ref[...], preferred_element_type=F32)
        normed = normed_by(mid, gain_ref[...]).astype(BF16)
        return mid, jnp.dot(normed, w_up_ref[...], preferred_element_type=F32)

    for n in range(pieces):
        mid, up = start(n)
        act = (0.5 * up * (1.0 + lax.erf(up * 0.5**0.5))).astype(BF16)
        out = mid + lax.dot_general(act, w_down_ref[...], NT, preferred_element_type=F32)
        held_ref[n * part : (n + 1) * part] = out.reshape(part, half, feats, width)
        if of_other:
            copy_out(held_ref, n, 1 - core)
    for copy in copies:
        copy.wait()


def vmem(count):
    return [pl.BlockSpec(memory_space=pltpu.VMEM)] * count


def limit(mib):
    return pltpu.CompilerParams(vmem_limit_bytes=mib << 20)


def body(
    cells, missing, feat_ids, feat_table, nan_embed, gain_one, w_qkv, w_out, gain_two, w_up, w_down
):
    chips = lax.axis_size("chip")
    all_rows, feats, width = cells.shape
    swap = [(0, 1), (1, 0)]
    halves = jax.ShapeDtypeStruct((all_rows // 2, feats, width), BF16)
    packed = jax.ShapeDtypeStruct((chips, all_rows * feats * width // (chips * LANES), LANES), BF16)
    hbm = pl.BlockSpec(memory_space=pltpu.HBM)
    own, other = pl.pallas_call(
        functools.partial(tokens_kernel, chips),
        out_shape=[halves] * 2,
        in_specs=[hbm] * 5,
        out_specs=vmem(2),
        scratch_shapes=[
            pltpu.VMEM(cells.shape, cells.dtype),
            pltpu.VMEM(missing.shape[::-1], missing.dtype),
            pltpu.VMEM(feat_table.shape, F32),
            pltpu.VMEM((1, width), F32),
            pltpu.SMEM(feat_ids.shape, feat_ids.dtype),
            pltpu.SemaphoreType.DMA((4 + PIECES,)),
        ],
        compiler_params=limit(12),
        name="tokens",
    )(*(pltpu.with_memory_space_constraint(x, pltpu.HBM) for x in (cells, missing.T, feat_table, nan_embed[None], feat_ids)))
    tokens = pl.pallas_call(
        merge_kernel,
        out_shape=packed,
        in_specs=vmem(2),
        out_specs=vmem(1)[0],
        compiler_params=limit(12),
        name="merge",
    )(own, lax.ppermute(other, "core", swap))
    tokens = lax.all_to_all(tokens, "chip", 0, 0, tiled=True)
    context = pl.pallas_call(
        functools.partial(attention_kernel, feats),
        out_shape=packed,
        in_specs=vmem(3),
        out_specs=vmem(1)[0],
        compiler_params=limit(24),
        name="attend",
    )(tokens, gain_one[None], w_qkv)
    context = lax.all_to_all(context, "chip", 0, 0, tiled=True)
    swapped = lax.ppermute(context, "core", swap)
    half = all_rows // chips // 2
    both = jax.ShapeDtypeStruct((chips, 2, half, feats, width), F32)
    one = jax.ShapeDtypeStruct((chips, half, feats, width), F32)

    def finish(of_other, base, context, *before):
        scratch = [pltpu.VMEM(one.shape, F32), pltpu.SemaphoreType.DMA((2 * PIECES,))]
        return pl.pallas_call(
            functools.partial(finish_kernel, feats, of_other),
            out_shape=both if of_other else one,
            in_specs=vmem(6 + len(before)),
            out_specs=hbm if of_other else vmem(1)[0],
            scratch_shapes=scratch if of_other else [],
            compiler_params=limit(16),
            cost_estimate=pl.CostEstimate(flops=10**9, bytes_accessed=2 * 10**6, transcendentals=0),
            name="finish",
        )(base, context, w_out, gain_two[None], w_up, w_down.T, *before)

    return finish(1, other, swapped, finish(0, own, context)).reshape(cells.shape)


def solution(mesh):
    chips = mesh.shape["feat"] // 2
    split = Mesh(mesh.devices.reshape(mesh.shape["groups"], chips, 2), ALL)
    in_specs = (P("groups", FEAT, None), P("groups", FEAT), P(ALL)) + (P(),) * 8
    return jax.shard_map(
        body, mesh=split, in_specs=in_specs, out_specs=P("groups", FEAT, None), check_vma=False
    )
```

```python
import functools

import jax
import jax.numpy as jnp
from jax import lax
from jax.experimental import pallas as pl
from jax.experimental.pallas import tpu as pltpu
from jax.sharding import Mesh
from jax.sharding import PartitionSpec as P

HEADS = 6
LANES = 128
ONES = 16
LEAD, LAG = 2,1
EARLY = 1
HOLD_NS = 27000
PIECES = 4
FEAT = ("chip", "core")
ALL = ("groups", "chip", "core")
F32 = jnp.float32
BF16 = jnp.bfloat16
NT = (((1,), (1,)), ((), ()))
TT = (((0,), (1,)), ((), ()))


def normed_by(values, gain):
    width = values.shape[-1]
    mean = jnp.sum(values, axis=-1, keepdims=True) * (1.0 / width)
    centered = values - mean
    var = jnp.sum(centered * centered, axis=-1, keepdims=True) * (1.0 / width)
    return centered * lax.rsqrt(var + 1e-05) * gain


def tokens_kernel(
    chips, cells_hbm, missing_hbm, table_hbm, nan_hbm, ids_hbm, own_ref, other_ref,
    cells_ref, missing_ref, table_ref, nan_ref, ids_ref, sems
):
    feats = cells_ref.shape[1]
    rows = cells_ref.shape[0] // chips
    half = rows // 2
    part = cells_ref.shape[0] // PIECES
    core = lax.axis_index("core")
    small = [
        pltpu.make_async_copy(*pair, sems.at[n])
        for n, pair in enumerate(
            [(ids_hbm, ids_ref), (table_hbm, table_ref), (missing_hbm, missing_ref), (nan_hbm, nan_ref)]
        )
    ]
    large = [
        pltpu.make_async_copy(
            cells_hbm.at[pl.ds(n * part, part)], cells_ref.at[pl.ds(n * part, part)], sems.at[len(small) + n]
        )
        for n in range(PIECES)
    ]
    for copy in small + large:
        copy.start()
    for copy in small:
        copy.wait()
    femb = jnp.concatenate([table_ref[pl.ds(ids_ref[f], 1), :] for f in range(feats)], axis=0)
    nan = nan_ref[...]
    low = missing_ref[...].astype(F32)
    high = jnp.concatenate([low[:, half:], low[:, :half]], axis=1)
    columns = [jnp.where(c == 0, low, high) for c in (core, 1 - core)]
    for c in range(chips):
        if c % (chips // PIECES) == 0:
            large[c // (chips // PIECES)].wait()
        for of_core, column, out_ref in ((core, columns[0], own_ref), (1 - core, columns[1], other_ref)):
            for i in range(half):
                lane = c * rows + i
                cell = cells_ref[lane + of_core * half].astype(F32)
                out_ref[c * half + i] = (cell + column[:, lane : lane + 1] * nan + femb).astype(BF16)


def merge_kernel(own_ref, other_ref, out_ref):
    chips = out_ref.shape[0]
    half = own_ref.shape[0] // chips
    feats = own_ref.shape[1]

    @pl.when(lax.axis_index("core") == 1)
    def _():
        pl.delay(HOLD_NS)

    for c in range(chips):
        for i in range(half):
            own = own_ref[c * half + i].astype(F32)
            other = other_ref[c * half + i].astype(F32)
            low = jnp.concatenate([own[:, :LANES], other[:, :LANES]], axis=0).astype(BF16)
            high = jnp.concatenate([own[:, LANES:], other[:, LANES:]], axis=1).astype(BF16)
            out_ref[c, 3 * i * feats : (3 * i + 2) * feats, :] = low
            out_ref[c, (3 * i + 2) * feats : (3 * i + 3) * feats, :] = high


def attention_kernel(feats, in_ref, gain_ref, w_ref, out_ref):
    width = gain_ref.shape[-1]
    head_dim = width // HEADS
    chips = in_ref.shape[0]
    cells = chips * feats
    split = LANES // 2
    head_of = lax.broadcasted_iota(jnp.int32, (1, width), 1) // head_dim
    scale = head_dim**-0.5 * 1.4426950408889634
    gain = gain_ref[...]

    def tile(i, t):
        return pl.ds(pl.multiple_of((3 * i + t) * feats, feats), feats)

    def flat(i, t):
        return in_ref[:, tile(i, t), :].astype(F32).reshape(cells, LANES)

    def scores_of(q, k, h):
        mine = jnp.where(head_of == h, q, jnp.zeros_like(q))
        return lax.dot_general(k, mine, NT, preferred_element_type=F32)

    def softmax(s):
        top = jnp.max(s, axis=0, keepdims=True)
        return jnp.exp2((s - top) * scale).astype(BF16)

    def context_of(v, expo, h):
        mine = v[h * head_dim : (h + 1) * head_dim]
        mine = jnp.concatenate([mine, jnp.ones((ONES, 2 * cells), BF16)], axis=0)
        part = jnp.dot(mine, expo, preferred_element_type=F32)
        return part[:head_dim] * (1.0 / part[head_dim : head_dim + 1])

    def ready(i):
        high = flat(i, 2)
        values = jnp.concatenate(
            [
                jnp.concatenate([flat(i, side), high[:, side * split : (side + 1) * split]], axis=1)
                for side in range(2)
            ],
            axis=0,
        )
        normed = normed_by(values, gain).astype(BF16)
        q = jnp.dot(normed, w_ref[:, :width], preferred_element_type=F32).astype(BF16)
        k = jnp.dot(normed, w_ref[:, width : 2 * width], preferred_element_type=F32).astype(BF16)
        v = lax.dot_general(w_ref[:, 2 * width :], normed, TT, preferred_element_type=F32).astype(BF16)
        return (q[:cells], q[cells:]), k, v

    def put(i, done):
        highs = []
        for side in range(2):
            rest = jnp.zeros((2 * LANES - width, cells), F32)
            context = jnp.concatenate([*done[side], rest], axis=0).T
            out_ref[:, tile(i, side), :] = context[:, :LANES].reshape(chips, feats, LANES).astype(BF16)
            highs.append(context[:, LANES:width])
        high = jnp.concatenate(highs, axis=1).reshape(chips, feats, LANES)
        out_ref[:, tile(i, 2), :] = high.astype(BF16)

    count = in_ref.shape[1] // (3 * feats)
    units = [(i, h, side) for i in range(count) for h in range(HEADS) for side in range(2)]
    made = {0: ready(0)}
    done = {(i, side): [] for i in range(count) for side in range(2)}
    ahead, expos = [], []

    def issue(n):
        i, h, side = units[n]
        ahead.append(scores_of(made[i][0][side], made[i][1], h))

    def retire(n):
        i, h, side = units[n]
        done[i, side].append(context_of(made[i][2], expos.pop(0), h))
        if (h, side) == (HEADS - 1, 1):
            put(i, [done[i, 0], done[i, 1]])

    for n in range(LEAD):
        issue(n)
    for n, (i, h, side) in enumerate(units):
        if (h, side) == (EARLY, 0) and i + 1 < count:
            made[i + 1] = ready(i + 1)
        if n + LEAD < len(units):
            issue(n + LEAD)
        expos.append(softmax(ahead.pop(0)))
        if n >= LAG:
            retire(n - LAG)
    for n in range(len(units) - LAG, len(units)):
        retire(n)


def finish_kernel(
    feats, of_other, base_ref, context_ref, w_out_ref, gain_ref, w_up_ref, w_down_ref, *rest
):
    width = gain_ref.shape[-1]
    chips = context_ref.shape[0]
    half = context_ref.shape[1] // (3 * feats)
    split = LANES // 2
    core = lax.axis_index("core")
    pieces = 2
    part = chips // pieces
    copies = []

    def copy_out(source, n, of_core):
        at = pl.ds(n * part, part)
        copies.append(pltpu.make_async_copy(source.at[at], out_hbm.at[at, of_core], sems.at[len(copies)]))
        copies[-1].start()

    if of_other:
        first_ref, out_hbm, held_ref, sems = rest
        copies.append(pltpu.make_async_copy(first_ref, out_hbm.at[:, core], sems.at[0]))
        copies[0].start()
    else:
        (held_ref,) = rest

    def start(n):
        tiles = context_ref[n * part : (n + 1) * part].astype(F32).reshape(part, half, 3, feats, LANES)
        high = tiles[:, :, 2, :, of_other * split : (of_other + 1) * split]
        context = jnp.concatenate([tiles[:, :, of_other], high], axis=-1).reshape(-1, width)
        base = base_ref[n * part * half : (n + 1) * part * half].astype(F32).reshape(-1, width)
        mid = base + jnp.dot(context.astype(BF16), w_out_ref[...], preferred_element_type=F32)
        normed = normed_by(mid, gain_ref[...]).astype(BF16)
        return mid, jnp.dot(normed, w_up_ref[...], preferred_element_type=F32)

    for n in range(pieces):
        mid, up = start(n)
        act = (0.5 * up * (1.0 + lax.erf(up * 0.5**0.5))).astype(BF16)
        out = mid + lax.dot_general(act, w_down_ref[...], NT, preferred_element_type=F32)
        held_ref[n * part : (n + 1) * part] = out.reshape(part, half, feats, width)
        if of_other:
            copy_out(held_ref, n, 1 - core)
    for copy in copies:
        copy.wait()


def vmem(count):
    return [pl.BlockSpec(memory_space=pltpu.VMEM)] * count


def limit(mib):
    return pltpu.CompilerParams(vmem_limit_bytes=mib << 20)


def body(
    cells, missing, feat_ids, feat_table, nan_embed, gain_one, w_qkv, w_out, gain_two, w_up, w_down
):
    chips = lax.axis_size("chip")
    all_rows, feats, width = cells.shape
    swap = [(0, 1), (1, 0)]
    halves = jax.ShapeDtypeStruct((all_rows // 2, feats, width), BF16)
    packed = jax.ShapeDtypeStruct((chips, all_rows * feats * width // (chips * LANES), LANES), BF16)
    hbm = pl.BlockSpec(memory_space=pltpu.HBM)
    own, other = pl.pallas_call(
        functools.partial(tokens_kernel, chips),
        out_shape=[halves] * 2,
        in_specs=[hbm] * 5,
        out_specs=vmem(2),
        scratch_shapes=[
            pltpu.VMEM(cells.shape, cells.dtype),
            pltpu.VMEM(missing.shape[::-1], missing.dtype),
            pltpu.VMEM(feat_table.shape, F32),
            pltpu.VMEM((1, width), F32),
            pltpu.SMEM(feat_ids.shape, feat_ids.dtype),
            pltpu.SemaphoreType.DMA((4 + PIECES,)),
        ],
        compiler_params=limit(12),
        name="tokens",
    )(*(pltpu.with_memory_space_constraint(x, pltpu.HBM) for x in (cells, missing.T, feat_table, nan_embed[None], feat_ids)))
    tokens = pl.pallas_call(
        merge_kernel,
        out_shape=packed,
        in_specs=vmem(2),
        out_specs=vmem(1)[0],
        compiler_params=limit(12),
        name="merge",
    )(own, lax.ppermute(other, "core", swap))
    tokens = lax.all_to_all(tokens, "chip", 0, 0, tiled=True)
    context = pl.pallas_call(
        functools.partial(attention_kernel, feats),
        out_shape=packed,
        in_specs=vmem(3),
        out_specs=vmem(1)[0],
        compiler_params=limit(24),
        name="attend",
    )(tokens, gain_one[None], w_qkv)
    context = lax.all_to_all(context, "chip", 0, 0, tiled=True)
    swapped = lax.ppermute(context, "core", swap)
    half = all_rows // chips // 2
    both = jax.ShapeDtypeStruct((chips, 2, half, feats, width), F32)
    one = jax.ShapeDtypeStruct((chips, half, feats, width), F32)

    def finish(of_other, base, context, *before):
        scratch = [pltpu.VMEM(one.shape, F32), pltpu.SemaphoreType.DMA((2 * PIECES,))]
        return pl.pallas_call(
            functools.partial(finish_kernel, feats, of_other),
            out_shape=both if of_other else one,
            in_specs=vmem(6 + len(before)),
            out_specs=hbm if of_other else vmem(1)[0],
            scratch_shapes=scratch if of_other else [],
            compiler_params=limit(16),
            cost_estimate=pl.CostEstimate(flops=10**9, bytes_accessed=2 * 10**6, transcendentals=0),
            name="finish",
        )(base, context, w_out, gain_two[None], w_up, w_down.T, *before)

    return finish(1, other, swapped, finish(0, own, context)).reshape(cells.shape)


def solution(mesh):
    chips = mesh.shape["feat"] // 2
    split = Mesh(mesh.devices.reshape(mesh.shape["groups"], chips, 2), ALL)
    in_specs = (P("groups", FEAT, None), P("groups", FEAT), P(ALL)) + (P(),) * 8
    return jax.shard_map(
        body, mesh=split, in_specs=in_specs, out_specs=P("groups", FEAT, None), check_vma=False
    )
```
